32 devices in a mesh: vocab: 8 (over z, y), dp: 4 (over x, core).
Axes of the slice: x: 2, y: 2, z: 4, core: 2. Of those that a mesh axis runs over, the one named last changes fastest.
Arguments:
- hidden: bfloat16 [2, 128, 7168], P(None, ('vocab', 'dp')), may hold values from -18 to 18
- unembed: bfloat16 [7168, 8192], P(None, ('vocab', 'dp')), may hold values from -0.24803919 to 0.24803919
- targets: int32 [2, 128], replicated, may hold values from 0 to 8191
Outputs:
- token_loss: float32 [2, 128], P(None, ('vocab', 'dp'))
- total_loss: float32 [], replicated
The draws below stay inside these ranges and needn't reach their ends.
All inputs are finite; a program needn't handle non-finite values.
Results may differ from the reference program's by a relative error of at most 0.0003.
Values may be sent and summed in bfloat16 or wider, within the bound.
No kernel may reach another device: no remote copies, remote signals or barrier semaphores. Data moves between devices by JAX's collectives and lax.ppermute only.
A program may use at most 128 MiB of HBM per device.

```python
import math
import jax
import jax.numpy as jnp
import numpy as np
from jax import lax

D = 7168
V_DEV = 256
VOCAB = 8192
TOKENS = 128


def draw_unembed(key, part):
    spread = 3.0 / math.sqrt(D)
    normals = jax.random.normal(jax.random.fold_in(key, 913), (D, VOCAB), jnp.float32)
    weight = jnp.clip(normals, -6.0, 6.0) * spread
    return weight.astype(jnp.bfloat16)


def draw_hidden(key, part):
    rising = 1.0 + 2.0 * jnp.arange(TOKENS, dtype=jnp.float32) / TOKENS
    normals = jax.random.normal(jax.random.fold_in(key, 917), (2, TOKENS, D), jnp.float32)
    values = jnp.clip(normals, -6.0, 6.0) * rising[None, :, None]
    return values.astype(jnp.bfloat16)


def plant(result, key, low, top_value):
    shape = result.shape
    place = [jax.random.randint(jax.random.fold_in(key, axis), (), 0, shape[axis]) for axis in range(len(shape))]
    result = result.at[tuple(place)].set(low)
    longest = shape.index(max(shape))
    place[longest] = (place[longest] + 1) % shape[longest]
    return result.at[tuple(place)].set(top_value)


def rank_bounds(amount, slope):
    portions = [(1 << 20) // math.isqrt(standing ** slope) + 1 for standing in range(1, amount + 1)]
    scale = 1 + sum(portions) // (1 << 30)
    return np.cumsum(np.array([max(1, weight // scale) for weight in portions]))


def ranked_ids(stream_key, extent, amount, slope):
    listing = rank_bounds(amount, slope)
    lot = jax.random.randint(jax.random.fold_in(stream_key, 1), extent, 0, int(listing[amount - 1]))
    standing = jnp.searchsorted(jnp.asarray(listing, jnp.int32), lot, side="right")
    return jax.random.permutation(jax.random.fold_in(stream_key, 2), amount)[standing].astype(jnp.int32)


def setup_inputs(seed: int = 0) -> dict:
    seeds = jax.random.split(jax.random.key(seed), 4)
    return {
        "hidden": draw_hidden(jax.random.fold_in(seeds[3], 71), 0),
        "unembed": draw_unembed(jax.random.fold_in(seeds[3], 71), 0),
        "targets": plant(ranked_ids(seeds[2], (2, TOKENS), VOCAB, 2), jax.random.fold_in(seeds[2], 3), 0, VOCAB - 1).astype(jnp.int32),
    }


FLOOR_VALUE = -1.0e30
MTP_WEIGHT = 0.3


def join_stats(earlier, later):
    highest = jnp.maximum(earlier[0], later[0])
    exp_total = earlier[1] * jnp.exp(earlier[0] - highest) + later[1] * jnp.exp(later[0] - highest)
    return highest, exp_total, earlier[2] + later[2]


def reference(hidden, unembed, targets):
    row_block = hidden.astype(jnp.float32)
    block_count = unembed.shape[1] // V_DEV

    def absorb(running, block_index):
        offset = (block_index * V_DEV).astype(jnp.int32)
        columns = lax.dynamic_slice_in_dim(unembed, offset, V_DEV, 1).astype(jnp.float32)
        logits = jnp.einsum("srd,dc->src", row_block, columns, precision=lax.Precision.HIGHEST)
        highest = jnp.max(logits, axis=2)
        exp_total = jnp.sum(jnp.exp(logits - highest[:, :, None]), axis=2)
        column_ids = offset + lax.broadcasted_iota(jnp.int32, logits.shape, 2)
        picked = jnp.sum(jnp.where(column_ids == targets[:, :, None], logits, 0.0), axis=2)
        return join_stats(running, (highest, exp_total, picked)), None

    start_state = (jnp.full((2, TOKENS), FLOOR_VALUE, jnp.float32), jnp.zeros((2, TOKENS), jnp.float32), jnp.zeros((2, TOKENS), jnp.float32))
    final_state, _ = lax.scan(absorb, start_state, jnp.arange(block_count, dtype=jnp.int32))
    token_loss = final_state[0] + jnp.log(final_state[1]) - final_state[2]
    total_loss = jnp.sum(token_loss[0]) / TOKENS + MTP_WEIGHT * jnp.sum(token_loss[1]) / TOKENS
    return token_loss, total_loss
```

```python
import functools
import jax
import jax.numpy as jnp
from jax import lax
from jax.experimental import pallas as pl
from jax.experimental.pallas import tpu as pltpu
from jax.sharding import Mesh, PartitionSpec as P

MTP_WEIGHT = 0.3
AXES = ("vocab", "chip", "core")
CHIPS = ("vocab", "chip")


def bits(count):
    return [1 << place for place in range(count.bit_length() - 1)]


def gather_orders(n_vocab, n_chip):
    near = bits(n_chip) + [n_chip * mask for mask in bits(n_vocab)[:1]]
    far = [n_chip * mask for mask in bits(n_vocab)[1:]]
    return (far[::-1] + near, far + near[::-1])


def exchange(value, masks, n_chips):
    pairs = [(2 * chip + core, 2 * (chip ^ masks[core]) + core) for chip in range(n_chips) for core in range(2)]
    return lax.ppermute(value, AXES, pairs)


def to_other_core(value, n_chips):
    pairs = [(source, source ^ 1) for source in range(2 * n_chips)]
    return lax.ppermute(value, AXES, pairs)


def offset(masks, place):
    total = 0
    for number, mask in enumerate(masks):
        if place >> number & 1:
            total ^= mask
    return total


def stats_kernel(orders, block, n_chip, wanted, kept, arrived, own, other, out, logits):
    core = lax.axis_index("core")
    chip = lax.axis_index("vocab") * n_chip + lax.axis_index("chip")
    width = own.shape[1]
    blocks = kept.shape[0] // block
    for part, rows in enumerate((kept, arrived)):
        for side, columns in enumerate((own, other)):
            product = jnp.dot(rows[...], columns[...], preferred_element_type=jnp.float32)
            for number in range(blocks):
                place = part * blocks + number
                shift = jnp.where(core == 0, offset(orders[0], place), offset(orders[1], place))
                first = pl.multiple_of((chip ^ shift) * block, block)
                logits[pl.ds(first, block), pl.ds(side * width, width)] = product[number * block : (number + 1) * block]
    values = logits[...]
    highest = jnp.max(values, axis=1, keepdims=True)
    exp_total = jnp.sum(jnp.exp(values - highest), axis=1, keepdims=True)
    device = 2 * chip + core
    lane = lax.broadcasted_iota(jnp.int32, values.shape, 1)
    column_ids = jnp.where(lane < width, device * width + lane, (device ^ 1) * width + lane - width)
    picked = jnp.sum(jnp.where(column_ids == wanted[...], values, 0.0), axis=1, keepdims=True)
    member = lax.broadcasted_iota(jnp.int32, (values.shape[0], 128), 1)
    table = jnp.where(member == 0, highest, jnp.where(member == 1, exp_total, picked))
    sent = jnp.transpose(table)[:8]
    for chip_number in range(out.shape[0]):
        out[chip_number] = sent


def loss_kernel(n_chip, block, heads_rows, received, own_loss, part):
    chip = lax.axis_index("vocab") * n_chip + lax.axis_index("chip")
    rows = received.shape[2]
    highs = received[:, 0, :]
    highest = jnp.max(highs, axis=0, keepdims=True)
    exp_total = jnp.sum(received[:, 1, :] * jnp.exp(highs - highest), axis=0, keepdims=True)
    picked = jnp.sum(received[:, 2, :], axis=0, keepdims=True)
    loss = highest + jnp.log(exp_total) - picked
    lane = lax.broadcasted_iota(jnp.int32, loss.shape, 1)
    weight = jnp.where(lane // heads_rows % 2 == 0, 1.0 / rows, MTP_WEIGHT / rows)
    part[...] = jnp.broadcast_to(jnp.sum(loss * weight, axis=1, keepdims=True), part.shape)
    turned = pltpu.roll(jnp.broadcast_to(loss, (8, rows)), rows - chip * block, 1)
    own_loss[...] = turned[:, :128]


def local(hidden, unembed, targets):
    heads, tok_rows, depth = hidden.shape
    block = heads * tok_rows
    width = unembed.shape[1]
    n_vocab, n_chip = lax.axis_size("vocab"), lax.axis_size("chip")
    n_chips = n_vocab * n_chip
    orders = gather_orders(n_vocab, n_chip)
    core = lax.axis_index("core")
    rows = n_chips * block

    other_columns = to_other_core(unembed, n_chips)
    kept = hidden.reshape(block, depth)
    for number in range(len(orders[0])):
        arrived = exchange(kept, (orders[0][number], orders[1][number]), n_chips)
        if number < len(orders[0]) - 1:
            kept = jnp.concatenate([kept, arrived], axis=0)
    mine = lax.dynamic_index_in_dim(targets.reshape(heads, n_chips, 2, tok_rows), core, 2, keepdims=False)
    wanted = jnp.transpose(mine, (1, 0, 2)).reshape(rows, 1)
    held = 2 * (rows + 2 * width) * depth + 4 * rows * (4 * width + 2 * 128 + 8 * n_chips)
    sent = pl.pallas_call(
        functools.partial(stats_kernel, orders, block, n_chip),
        out_shape=jax.ShapeDtypeStruct((n_chips, 8, rows), jnp.float32),
        scratch_shapes=[pltpu.VMEM((rows, 2 * width), jnp.float32)],
        cost_estimate=pl.CostEstimate(flops=4 * rows * width * depth, bytes_accessed=4 * (rows + width) * depth, transcendentals=0),
        compiler_params=pltpu.CompilerParams(vmem_limit_bytes=held + 2**21),
        name="stats",
    )(wanted, kept, arrived, unembed, other_columns)
    received = lax.all_to_all(sent, CHIPS, split_axis=0, concat_axis=0, tiled=True)
    own_loss, part = pl.pallas_call(
        functools.partial(loss_kernel, n_chip, block, tok_rows),
        out_shape=(jax.ShapeDtypeStruct((8, 128), jnp.float32), jax.ShapeDtypeStruct((8, 128), jnp.float32)),
        compiler_params=pltpu.CompilerParams(vmem_limit_bytes=2**20 + 4 * 4 * n_chips * 8 * rows),
        name="loss",
    )(received)
    token_loss = own_loss[0, :block].reshape(heads, tok_rows)
    total = part[0, 0] + to_other_core(part, n_chips)[0, 0]
    return token_loss, total


def solution(mesh):
    n_vocab, n_data = mesh.shape["vocab"], mesh.shape["dp"]
    fine = Mesh(mesh.devices.reshape(n_vocab, n_data // 2, 2), AXES)
    return jax.shard_map(
        local,
        mesh=fine,
        in_specs=(P(None, AXES, None), P(None, AXES), P()),
        out_specs=(P(None, AXES), P()),
        check_vma=False,
    )
```

```python
import functools
import jax
import jax.numpy as jnp
from jax import lax
from jax.experimental import pallas as pl
from jax.experimental.pallas import tpu as pltpu
from jax.sharding import Mesh, PartitionSpec as P

MTP_WEIGHT = 0.3
AXES = ("vocab", "chip", "core")
CHIPS = ("vocab", "chip")


def bits(count):
    return [1 << place for place in range(count.bit_length() - 1)]


def gather_orders(n_vocab, n_chip):
    near = bits(n_chip) + [n_chip * mask for mask in bits(n_vocab)[:1]]
    far = [n_chip * mask for mask in bits(n_vocab)[1:]]
    return (
        (far[::-1] + near, far + near[::-1]),
        (near + far[::-1], near[::-1] + far),
    )


def exchange(value, masks, n_chips):
    pairs = [(2 * chip + core, 2 * (chip ^ masks[core]) + core) for chip in range(n_chips) for core in range(2)]
    return lax.ppermute(value, AXES, pairs)


def to_other_core(value, n_chips):
    pairs = [(source, source ^ 1) for source in range(2 * n_chips)]
    return lax.ppermute(value, AXES, pairs)


def offset(masks, place):
    total = 0
    for number, mask in enumerate(masks):
        if place >> number & 1:
            total ^= mask
    return total


def add_products(orders, block, part, n_chip, rows, columns, first_depth, logits):
    core = lax.axis_index("core")
    chip = lax.axis_index("vocab") * n_chip + lax.axis_index("chip")
    blocks = rows.shape[0] // block
    depth = pl.ds(first_depth, rows.shape[1])
    for side, column in enumerate(columns):
        width = column.shape[1]
        product = jnp.dot(rows[...], column[depth, :], preferred_element_type=jnp.float32)
        for number in range(blocks):
            place = part * blocks + number
            shift = jnp.where(core == 0, offset(orders[0], place), offset(orders[1], place))
            first = pl.multiple_of((chip ^ shift) * block, block)
            target = (pl.ds(first, block), pl.ds(side * width, width))
            logits[target] = logits[target] + product[number * block : (number + 1) * block]


def kept_kernel(flows, block, n_chip, kept_a, kept_b, own, other, own_out, other_out, logits, arrivals):
    cut, depth = kept_a.shape[1], own.shape[0]
    pieces = ((0, cut), (cut, depth - cut))
    copies = []
    for number, (first, count) in enumerate(pieces):
        for side, (source, target) in enumerate(((own, own_out), (other, other_out))):
            span = pl.ds(first, count)
            copies.append(pltpu.make_async_copy(source.at[span], target.at[span], arrivals.at[2 * number + side]))
    for copy in copies:
        copy.start()
    logits[...] = jnp.zeros_like(logits)
    for number, kept in enumerate((kept_a, kept_b)):
        copies[2 * number].wait()
        copies[2 * number + 1].wait()
        add_products(flows[number], block, 0, n_chip, kept, (own_out, other_out), pieces[number][0], logits)


def stats_kernel(flows, block, n_chip, wanted, arrived_a, arrived_b, own, other, partial, out, logits):
    core = lax.axis_index("core")
    chip = lax.axis_index("vocab") * n_chip + lax.axis_index("chip")
    width = own.shape[1]
    logits[...] = partial[...]
    add_products(flows[0], block, 1, n_chip, arrived_a, (own, other), 0, logits)
    add_products(flows[1], block, 1, n_chip, arrived_b, (own, other), arrived_a.shape[1], logits)
    values = logits[...]
    highest = jnp.max(values, axis=1, keepdims=True)
    exp_total = jnp.sum(jnp.exp(values - highest), axis=1, keepdims=True)
    device = 2 * chip + core
    lane = lax.broadcasted_iota(jnp.int32, values.shape, 1)
    column_ids = jnp.where(lane < width, device * width + lane, (device ^ 1) * width + lane - width)
    picked = jnp.sum(jnp.where(column_ids == wanted[...], values, 0.0), axis=1, keepdims=True)
    member = lax.broadcasted_iota(jnp.int32, (values.shape[0], 128), 1)
    table = jnp.where(member == 0, highest, jnp.where(member == 1, exp_total, picked))
    sent = jnp.transpose(table)[:8]
    for chip_number in range(out.shape[0]):
        out[chip_number] = sent


def loss_kernel(n_chip, block, heads_rows, received, own_loss, part):
    chip = lax.axis_index("vocab") * n_chip + lax.axis_index("chip")
    rows = received.shape[2]
    highs = received[:, 0, :]
    highest = jnp.max(highs, axis=0, keepdims=True)
    exp_total = jnp.sum(received[:, 1, :] * jnp.exp(highs - highest), axis=0, keepdims=True)
    picked = jnp.sum(received[:, 2, :], axis=0, keepdims=True)
    loss = highest + jnp.log(exp_total) - picked
    lane = lax.broadcasted_iota(jnp.int32, loss.shape, 1)
    weight = jnp.where(lane // heads_rows % 2 == 0, 1.0 / rows, MTP_WEIGHT / rows)
    part[...] = jnp.broadcast_to(jnp.sum(loss * weight, axis=1, keepdims=True), part.shape)
    turned = pltpu.roll(jnp.broadcast_to(loss, (8, rows)), rows - chip * block, 1)
    own_loss[...] = turned[:, :128]


def local(hidden, unembed, targets):
    heads, tok_rows, depth = hidden.shape
    block = heads * tok_rows
    width = unembed.shape[1]
    n_vocab, n_chip = lax.axis_size("vocab"), lax.axis_size("chip")
    n_chips = n_vocab * n_chip
    flows = gather_orders(n_vocab, n_chip)
    core = lax.axis_index("core")
    rows = n_chips * block

    other_columns = to_other_core(unembed, n_chips)
    cut = depth // 128 * 2 // 3 * 128
    own_rows = hidden.reshape(block, depth)
    kept = [own_rows[:, :cut], own_rows[:, cut:]]
    arrived = [None, None]
    stages = len(flows[0][0])
    for number in range(stages):
        for flow in range(2):
            masks = (flows[flow][0][number], flows[flow][1][number])
            arrived[flow] = exchange(kept[flow], masks, n_chips)
        if number < stages - 1:
            for flow in range(2):
                kept[flow] = jnp.concatenate([kept[flow], arrived[flow]], axis=0)
    mine = lax.dynamic_index_in_dim(targets.reshape(heads, n_chips, 2, tok_rows), core, 2, keepdims=False)
    wanted = jnp.transpose(mine, (1, 0, 2)).reshape(rows, 1)
    cost = pl.CostEstimate(
        flops=2 * rows * width * depth, bytes_accessed=(rows + 4 * width) * depth, transcendentals=0
    )
    held = 2 * (rows + 2 * width) * depth + 4 * rows * (8 * width + 2 * 128 + 8 * n_chips)
    params = pltpu.CompilerParams(vmem_limit_bytes=held + 2**21)
    in_vmem = pl.BlockSpec(memory_space=pltpu.VMEM)
    in_place = pl.BlockSpec(memory_space=pl.ANY)
    columns = jax.ShapeDtypeStruct(unembed.shape, unembed.dtype)
    own_near, other_near, partial = pl.pallas_call(
        functools.partial(kept_kernel, flows, block, n_chip),
        out_shape=(columns, columns, jax.ShapeDtypeStruct((rows, 2 * width), jnp.float32)),
        in_specs=[in_vmem, in_vmem, in_place, in_place],
        out_specs=(in_vmem, in_vmem, in_vmem),
        scratch_shapes=[pltpu.SemaphoreType.DMA((4,))],
        cost_estimate=cost,
        compiler_params=params,
        name="kept",
    )(kept[0], kept[1], unembed, other_columns)
    sent = pl.pallas_call(
        functools.partial(stats_kernel, flows, block, n_chip),
        out_shape=jax.ShapeDtypeStruct((n_chips, 8, rows), jnp.float32),
        scratch_shapes=[pltpu.VMEM((rows, 2 * width), jnp.float32)],
        cost_estimate=cost,
        compiler_params=params,
        name="stats",
    )(wanted, arrived[0], arrived[1], own_near, other_near, partial)
    received = lax.all_to_all(sent, CHIPS, split_axis=0, concat_axis=0, tiled=True)
    own_loss, part = pl.pallas_call(
        functools.partial(loss_kernel, n_chip, block, tok_rows),
        out_shape=(jax.ShapeDtypeStruct((8, 128), jnp.float32), jax.ShapeDtypeStruct((8, 128), jnp.float32)),
        compiler_params=pltpu.CompilerParams(vmem_limit_bytes=2**20 + 4 * 4 * n_chips * 8 * rows),
        name="loss",
    )(received)
    token_loss = own_loss[0, :block].reshape(heads, tok_rows)
    total = part[0, 0] + to_other_core(part, n_chips)[0, 0]
    return token_loss, total


def solution(mesh):
    n_vocab, n_data = mesh.shape["vocab"], mesh.shape["dp"]
    fine = Mesh(mesh.devices.reshape(n_vocab, n_data // 2, 2), AXES)
    return jax.shard_map(
        local,
        mesh=fine,
        in_specs=(P(None, AXES, None), P(None, AXES), P()),
        out_specs=(P(None, AXES), P()),
        check_vma=False,
    )
```

```python
import functools
import jax
import jax.numpy as jnp
from jax import lax
from jax.experimental import pallas as pl
from jax.experimental.pallas import tpu as pltpu
from jax.sharding import Mesh, PartitionSpec as P

MTP_WEIGHT = 0.3
AXES = ("vocab", "chip", "core")
CHIPS = ("vocab", "chip")


def bits(count):
    return [1 << place for place in range(count.bit_length() - 1)]


def gather_orders(n_vocab, n_chip):
    near = bits(n_chip) + [n_chip * mask for mask in bits(n_vocab)[:1]]
    far = [n_chip * mask for mask in bits(n_vocab)[1:]]
    return (
        (far[::-1] + near, far + near[::-1]),
        (near + far[::-1], near[::-1] + far),
    )


def exchange(value, masks, n_chips):
    pairs = [(2 * chip + core, 2 * (chip ^ masks[core]) + core) for chip in range(n_chips) for core in range(2)]
    return lax.ppermute(value, AXES, pairs)


def to_other_core(value, n_chips):
    pairs = [(source, source ^ 1) for source in range(2 * n_chips)]
    return lax.ppermute(value, AXES, pairs)


def offset(masks, place):
    total = 0
    for number, mask in enumerate(masks):
        if place >> number & 1:
            total ^= mask
    return total


def add_products(orders, block, part, n_chip, rows, columns, side, first_depth, logits):
    core = lax.axis_index("core")
    chip = lax.axis_index("vocab") * n_chip + lax.axis_index("chip")
    blocks, width = rows.shape[0] // block, columns.shape[1]
    product = jnp.dot(
        rows[...], columns[pl.ds(first_depth, rows.shape[1]), :], preferred_element_type=jnp.float32
    )
    for number in range(blocks):
        place = part * blocks + number
        shift = jnp.where(core == 0, offset(orders[0], place), offset(orders[1], place))
        first = pl.multiple_of((chip ^ shift) * block, block)
        target = (pl.ds(first, block), pl.ds(side * width, width))
        logits[target] = logits[target] + product[number * block : (number + 1) * block]


def kept_kernel(flows, block, n_chip, kept_a, kept_b, own, other, other_out, logits, arrivals):
    cut, depth = kept_a.shape[1], own.shape[0]
    flow_rows = ((kept_a, 0), (kept_b, cut))
    copies = []
    for number, (first, count) in enumerate(((0, cut), (cut, depth - cut))):
        span = pl.ds(first, count)
        copies.append(pltpu.make_async_copy(other.at[span], other_out.at[span], arrivals.at[number]))
    for copy in copies:
        copy.start()
    logits[...] = jnp.zeros_like(logits)
    for number, (kept, first) in enumerate(flow_rows):
        add_products(flows[number], block, 0, n_chip, kept, own, 0, first, logits)
    for number, (kept, first) in enumerate(flow_rows):
        copies[number].wait()
        add_products(flows[number], block, 0, n_chip, kept, other_out, 1, first, logits)


def first_kernel(flows, block, n_chip, arrived, own, other, partial, logits):
    logits[...] = partial[...]
    for side, columns in enumerate((own, other)):
        add_products(flows[0], block, 1, n_chip, arrived, columns, side, 0, logits)


def stats_kernel(flows, block, n_chip, wanted, arrived, own, other, partial, out, logits):
    core = lax.axis_index("core")
    chip = lax.axis_index("vocab") * n_chip + lax.axis_index("chip")
    width = own.shape[1]
    logits[...] = partial[...]
    for side, columns in enumerate((own, other)):
        add_products(flows[1], block, 1, n_chip, arrived, columns, side, own.shape[0] - arrived.shape[1], logits)
    values = logits[...]
    highest = jnp.max(values, axis=1, keepdims=True)
    exp_total = jnp.sum(jnp.exp(values - highest), axis=1, keepdims=True)
    device = 2 * chip + core
    lane = lax.broadcasted_iota(jnp.int32, values.shape, 1)
    column_ids = jnp.where(lane < width, device * width + lane, (device ^ 1) * width + lane - width)
    picked = jnp.sum(jnp.where(column_ids == wanted[...], values, 0.0), axis=1, keepdims=True)
    member = lax.broadcasted_iota(jnp.int32, (values.shape[0], 128), 1)
    table = jnp.where(member == 0, highest + jnp.log(exp_total), picked)
    sent = jnp.transpose(table)[:2]
    for chip_number in range(out.shape[0]):
        out[chip_number] = sent


def loss_kernel(n_chip, block, tok_rows, received, own_loss, part):
    chip = lax.axis_index("vocab") * n_chip + lax.axis_index("chip")
    rows = received.shape[2]
    log_sums = received[:, 0, :]
    highest = jnp.max(log_sums, axis=0, keepdims=True)
    exp_total = jnp.sum(jnp.exp(log_sums - highest), axis=0, keepdims=True)
    picked = jnp.sum(received[:, 1, :], axis=0, keepdims=True)
    loss = highest + jnp.log(exp_total) - picked
    lane = lax.broadcasted_iota(jnp.int32, loss.shape, 1)
    weight = jnp.where(lane // tok_rows % 2 == 0, 1.0 / rows, MTP_WEIGHT / rows)
    part[...] = jnp.sum(loss * weight, axis=1, keepdims=True)
    repeated = jnp.broadcast_to(loss, (8, rows))
    for head in range(2):
        turned = pltpu.roll(repeated, rows - chip * block - head * tok_rows, 1)
        own_loss[pl.ds(head, 1), :] = turned[:1, :tok_rows]


def local(hidden, unembed, targets):
    heads, tok_rows, depth = hidden.shape
    block = heads * tok_rows
    width = unembed.shape[1]
    n_vocab, n_chip = lax.axis_size("vocab"), lax.axis_size("chip")
    n_chips = n_vocab * n_chip
    flows = gather_orders(n_vocab, n_chip)
    core = lax.axis_index("core")
    rows = n_chips * block

    cut = depth // 128 * 2 // 3 * 128
    own_rows = hidden.reshape(block, depth)
    kept = [own_rows[:, :cut], own_rows[:, cut:]]
    arrived = [None, None]
    stages = len(flows[0][0])
    for number in range(stages):
        for flow in range(2):
            masks = (flows[flow][0][number], flows[flow][1][number])
            arrived[flow] = exchange(kept[flow], masks, n_chips)
        if number == 0:
            later_columns, _ = lax.optimization_barrier((unembed, arrived))
            other_columns = to_other_core(later_columns, n_chips)
        if number < stages - 1:
            for flow in range(2):
                kept[flow] = jnp.concatenate([kept[flow], arrived[flow]], axis=0)
    mine = lax.dynamic_index_in_dim(targets.reshape(heads, n_chips, 2, tok_rows), core, 2, keepdims=False)
    wanted = jnp.transpose(mine, (1, 0, 2)).reshape(rows, 1)
    cost = pl.CostEstimate(
        flops=2 * rows * width * depth, bytes_accessed=(rows + 4 * width) * depth, transcendentals=0
    )
    held = 2 * (rows + 2 * width) * depth + 4 * rows * (8 * width + 2 * 128 + 8 * n_chips)
    params = pltpu.CompilerParams(vmem_limit_bytes=held + 2**21)
    in_vmem = pl.BlockSpec(memory_space=pltpu.VMEM)
    in_hbm = pl.BlockSpec(memory_space=pltpu.HBM)
    columns = jax.ShapeDtypeStruct(unembed.shape, unembed.dtype)
    other_near, partial = pl.pallas_call(
        functools.partial(kept_kernel, flows, block, n_chip),
        out_shape=(columns, jax.ShapeDtypeStruct((rows, 2 * width), jnp.float32)),
        in_specs=[in_vmem, in_vmem, in_vmem, in_hbm],
        out_specs=(in_vmem, in_vmem),
        scratch_shapes=[pltpu.SemaphoreType.DMA((2,))],
        cost_estimate=cost,
        compiler_params=params,
        name="kept",
    )(kept[0], kept[1], unembed, other_columns)
    logits = jax.ShapeDtypeStruct((rows, 2 * width), jnp.float32)
    partial = pl.pallas_call(
        functools.partial(first_kernel, flows, block, n_chip),
        out_shape=logits,
        cost_estimate=cost,
        compiler_params=params,
        name="first",
    )(arrived[0], unembed, other_near, partial)
    sent = pl.pallas_call(
        functools.partial(stats_kernel, flows, block, n_chip),
        out_shape=jax.ShapeDtypeStruct((n_chips, 2, rows), jnp.float32),
        scratch_shapes=[pltpu.VMEM((rows, 2 * width), jnp.float32)],
        cost_estimate=cost,
        compiler_params=params,
        name="stats",
    )(wanted, arrived[1], unembed, other_near, partial)
    received = lax.all_to_all(sent, CHIPS, split_axis=0, concat_axis=0, tiled=True)
    token_loss, part = pl.pallas_call(
        functools.partial(loss_kernel, n_chip, block, tok_rows),
        out_shape=(jax.ShapeDtypeStruct((heads, tok_rows), jnp.float32), jax.ShapeDtypeStruct((1, 1), jnp.float32)),
        compiler_params=pltpu.CompilerParams(vmem_limit_bytes=2**20 + 4 * 4 * n_chips * 8 * rows),
        name="loss",
    )(received)
    total = (part + to_other_core(part, n_chips)).reshape(())
    return token_loss, total


def solution(mesh):
    n_vocab, n_data = mesh.shape["vocab"], mesh.shape["dp"]
    fine = Mesh(mesh.devices.reshape(n_vocab, n_data // 2, 2), AXES)
    return jax.shard_map(
        local,
        mesh=fine,
        in_specs=(P(None, AXES, None), P(None, AXES), P()),
        out_specs=(P(None, AXES), P()),
        check_vma=False,
    )
```

```python
import functools
import jax
import jax.numpy as jnp
from jax import lax
from jax.experimental import pallas as pl
from jax.experimental.pallas import tpu as pltpu
from jax.sharding import Mesh, PartitionSpec as P

MTP_WEIGHT = 0.3
AXES = ("vocab", "chip", "core")
CHIPS = ("vocab", "chip")


def bits(count):
    return [1 << place for place in range(count.bit_length() - 1)]


def gather_orders(n_vocab, n_chip):
    near = bits(n_chip) + [n_chip * mask for mask in bits(n_vocab)[:1]]
    far = [n_chip * mask for mask in bits(n_vocab)[1:]]
    return (
        (far[::-1] + near, far + near[::-1]),
        (near + far[::-1], near[::-1] + far),
    )


def exchange(value, masks, n_chips):
    pairs = [(2 * chip + core, 2 * (chip ^ masks[core]) + core) for chip in range(n_chips) for core in range(2)]
    return lax.ppermute(value, AXES, pairs)


def to_other_core(value, n_chips):
    pairs = [(source, source ^ 1) for source in range(2 * n_chips)]
    return lax.ppermute(value, AXES, pairs)


def offset(masks, place):
    total = 0
    for number, mask in enumerate(masks):
        if place >> number & 1:
            total ^= mask
    return total


def add_products(orders, block, part, n_chip, rows, columns, side, first_depth, logits):
    core = lax.axis_index("core")
    chip = lax.axis_index("vocab") * n_chip + lax.axis_index("chip")
    blocks, width = rows.shape[0] // block, columns.shape[1]
    product = jnp.dot(
        rows[...], columns[pl.ds(first_depth, rows.shape[1]), :], preferred_element_type=jnp.float32
    )
    for number in range(blocks):
        place = part * blocks + number
        shift = jnp.where(core == 0, offset(orders[0], place), offset(orders[1], place))
        first = pl.multiple_of((chip ^ shift) * block, block)
        target = (pl.ds(first, block), pl.ds(side * width, width))
        logits[target] = logits[target] + product[number * block : (number + 1) * block]


def load_kernel(source, target, arrival):
    copy = pltpu.make_async_copy(source, target, arrival)
    copy.start()
    copy.wait()


def join_kernel(kept, arrived, out):
    half = kept.shape[0]
    out[:half] = kept[...]
    out[half:] = arrived[...]


def kept_kernel(flows, block, n_chip, targets, kept_a, kept_b, own, other, logits, wanted):
    rows, tokens = wanted.shape[0], targets.shape[1]
    tok_rows = block // targets.shape[0]
    row = lax.broadcasted_iota(jnp.int32, (rows, tokens), 0)
    token = (2 * (row // block) + lax.axis_index("core")) * tok_rows + row % tok_rows
    ids = jnp.where(row // tok_rows % 2 == 0, targets[0:1, :], targets[1:2, :])
    here = token == lax.broadcasted_iota(jnp.int32, (rows, tokens), 1)
    wanted[...] = jnp.broadcast_to(jnp.sum(jnp.where(here, ids, 0), axis=1, keepdims=True), wanted.shape)
    logits[...] = jnp.zeros_like(logits)
    for number, (kept, first) in enumerate(((kept_a, 0), (kept_b, kept_a.shape[1]))):
        for side, columns in enumerate((own, other)):
            add_products(flows[number], block, 0, n_chip, kept, columns, side, first, logits)


def first_kernel(flows, block, n_chip, arrived, own, other, partial, logits):
    logits[...] = partial[...]
    for side, columns in enumerate((own, other)):
        add_products(flows[0], block, 1, n_chip, arrived, columns, side, 0, logits)


def stats_kernel(flows, block, n_chip, wanted, arrived, own, other, partial, out, logits):
    core = lax.axis_index("core")
    chip = lax.axis_index("vocab") * n_chip + lax.axis_index("chip")
    width = own.shape[1]
    logits[...] = partial[...]
    for side, columns in enumerate((own, other)):
        add_products(flows[1], block, 1, n_chip, arrived, columns, side, own.shape[0] - arrived.shape[1], logits)
    values = logits[...]
    highest = jnp.max(values, axis=1, keepdims=True)
    exp_total = jnp.sum(jnp.exp(values - highest), axis=1, keepdims=True)
    device = 2 * chip + core
    lane = lax.broadcasted_iota(jnp.int32, values.shape, 1)
    column_ids = jnp.where(lane < width, device * width + lane, (device ^ 1) * width + lane - width)
    picked = jnp.sum(jnp.where(column_ids == wanted[:, :1], values, 0.0), axis=1, keepdims=True)
    member = lax.broadcasted_iota(jnp.int32, (values.shape[0], 128), 1)
    table = jnp.where(member == 0, highest + jnp.log(exp_total), picked)
    sent = jnp.transpose(table)[:2]
    for chip_number in range(out.shape[0]):
        out[chip_number] = sent


def loss_kernel(n_chip, block, tok_rows, received, own_loss, part):
    chip = lax.axis_index("vocab") * n_chip + lax.axis_index("chip")
    rows = received.shape[2]
    log_sums = received[:, 0, :]
    highest = jnp.max(log_sums, axis=0, keepdims=True)
    exp_total = jnp.sum(jnp.exp(log_sums - highest), axis=0, keepdims=True)
    picked = jnp.sum(received[:, 1, :], axis=0, keepdims=True)
    loss = highest + jnp.log(exp_total) - picked
    lane = lax.broadcasted_iota(jnp.int32, loss.shape, 1)
    weight = jnp.where(lane // tok_rows % 2 == 0, 1.0 / rows, MTP_WEIGHT / rows)
    part[...] = jnp.broadcast_to(jnp.sum(loss * weight, axis=1, keepdims=True), part.shape)
    repeated = jnp.broadcast_to(loss, (8, rows))
    for head in range(2):
        turned = pltpu.roll(repeated, rows - chip * block - head * tok_rows, 1)
        own_loss[pl.ds(head, 1), :] = turned[:1, :tok_rows]


def load(columns):
    return pl.pallas_call(
        load_kernel,
        out_shape=jax.ShapeDtypeStruct(columns.shape, columns.dtype),
        in_specs=[pl.BlockSpec(memory_space=pltpu.HBM)],
        out_specs=pl.BlockSpec(memory_space=pltpu.VMEM),
        scratch_shapes=[pltpu.SemaphoreType.DMA],
        cost_estimate=pl.CostEstimate(flops=0, bytes_accessed=4 * columns.size, transcendentals=0),
        compiler_params=pltpu.CompilerParams(vmem_limit_bytes=2**20 + 2 * columns.size),
    )(columns)


def join(kept, arrived):
    rows, depth = kept.shape
    return pl.pallas_call(
        join_kernel,
        out_shape=jax.ShapeDtypeStruct((2 * rows, depth), kept.dtype),
        cost_estimate=pl.CostEstimate(flops=0, bytes_accessed=8 * kept.size, transcendentals=0),
        compiler_params=pltpu.CompilerParams(vmem_limit_bytes=2**20 + 8 * kept.size),
        name="join",
    )(kept, arrived)


def local(hidden, unembed, targets):
    heads, tok_rows, depth = hidden.shape
    block = heads * tok_rows
    width = unembed.shape[1]
    n_vocab, n_chip = lax.axis_size("vocab"), lax.axis_size("chip")
    n_chips = n_vocab * n_chip
    flows = gather_orders(n_vocab, n_chip)
    rows = n_chips * block

    other_columns = to_other_core(unembed, n_chips)
    cut = depth // 128 * 2 // 3 * 128
    own_rows = hidden.reshape(block, depth)
    kept = [own_rows[:, :cut], own_rows[:, cut:]]
    arrived = [None, None]
    stages = len(flows[0][0])
    for number in range(stages):
        for flow in range(2):
            masks = (flows[flow][0][number], flows[flow][1][number])
            arrived[flow] = exchange(kept[flow], masks, n_chips)
        if number < stages - 1:
            for flow in range(2):
                kept[flow] = join(kept[flow], arrived[flow])
    own_near, other_near = unembed, load(other_columns)
    cost = pl.CostEstimate(
        flops=2 * rows * width * depth, bytes_accessed=(rows + 4 * width) * depth, transcendentals=0
    )
    held = 2 * (rows + 2 * width) * depth + 4 * rows * (8 * width + 3 * rows + 8 * n_chips)
    params = pltpu.CompilerParams(vmem_limit_bytes=held + 2**21)
    logits = jax.ShapeDtypeStruct((rows, 2 * width), jnp.float32)
    partial, wanted = pl.pallas_call(
        functools.partial(kept_kernel, flows, block, n_chip),
        out_shape=(logits, jax.ShapeDtypeStruct((rows, 128), jnp.int32)),
        cost_estimate=cost,
        compiler_params=params,
        name="kept",
    )(targets, kept[0], kept[1], own_near, other_near)
    partial = pl.pallas_call(
        functools.partial(first_kernel, flows, block, n_chip),
        out_shape=logits,
        cost_estimate=cost,
        compiler_params=params,
        name="first",
    )(arrived[0], own_near, other_near, partial)
    sent = pl.pallas_call(
        functools.partial(stats_kernel, flows, block, n_chip),
        out_shape=jax.ShapeDtypeStruct((n_chips, 2, rows), jnp.float32),
        scratch_shapes=[pltpu.VMEM((rows, 2 * width), jnp.float32)],
        cost_estimate=cost,
        compiler_params=params,
        name="stats",
    )(wanted, arrived[1], own_near, other_near, partial)
    received = lax.all_to_all(sent, CHIPS, split_axis=0, concat_axis=0, tiled=True)
    token_loss, part = pl.pallas_call(
        functools.partial(loss_kernel, n_chip, block, tok_rows),
        out_shape=(jax.ShapeDtypeStruct((heads, tok_rows), jnp.float32), jax.ShapeDtypeStruct((8, 128), jnp.float32)),
        compiler_params=pltpu.CompilerParams(vmem_limit_bytes=2**20 + 4 * 4 * n_chips * 8 * rows),
        name="loss",
    )(received)
    total = (part + to_other_core(part, n_chips))[0, 0]
    return token_loss, total


def solution(mesh):
    n_vocab, n_data = mesh.shape["vocab"], mesh.shape["dp"]
    fine = Mesh(mesh.devices.reshape(n_vocab, n_data // 2, 2), AXES)
    return jax.shard_map(
        local,
        mesh=fine,
        in_specs=(P(None, AXES, None), P(None, AXES), P()),
        out_specs=(P(None, AXES), P()),
        check_vma=False,
    )
```

```python
import functools
import jax
import jax.numpy as jnp
from jax import lax
from jax.experimental import pallas as pl
from jax.experimental.pallas import tpu as pltpu
from jax.sharding import Mesh, PartitionSpec as P

MTP_WEIGHT = 0.3
AXIS = "device"


def bits(count):
    return [1 << place for place in range(count.bit_length() - 1)]


def gather_orders(n_vocab, n_chip):
    near = bits(n_chip) + [n_chip * mask for mask in bits(n_vocab)[:1]]
    far = [n_chip * mask for mask in bits(n_vocab)[1:]]
    return (
        (far[::-1] + near[::-1], far + near),
        (near + far[::-1], near[::-1] + far),
    )


def parity(chip, n_chips):
    odd = chip
    for place in range(1, n_chips.bit_length() - 1):
        odd = odd ^ (chip >> place)
    return odd & 1


def team_devices(n_chips):
    return [[2 * chip + (team ^ parity(chip, n_chips)) for chip in range(n_chips)] for team in range(2)]


def place_of(n_chips):
    device = lax.axis_index(AXIS)
    chip, core = device // 2, device % 2
    return device, chip, core ^ parity(chip, n_chips)


def exchange(value, masks, n_chips):
    teams = team_devices(n_chips)
    pairs = [(teams[team][chip], teams[team][chip ^ masks[team]]) for team in range(2) for chip in range(n_chips)]
    return lax.ppermute(value, AXIS, sorted(pairs))


def to_other_core(value, n_chips):
    pairs = [(source, source ^ 1) for source in range(2 * n_chips)]
    return lax.ppermute(value, AXIS, pairs)


def offset(masks, place):
    total = 0
    for number, mask in enumerate(masks):
        if place >> number & 1:
            total ^= mask
    return total


def add_products(orders, block, part, n_chips, rows, columns, side, first_depth, logits):
    _, chip, team = place_of(n_chips)
    blocks, width = rows.shape[0] // block, columns.shape[1]
    product = jnp.dot(
        rows[...], columns[pl.ds(first_depth, rows.shape[1]), :], preferred_element_type=jnp.float32
    )
    for number in range(blocks):
        place = part * blocks + number
        shift = jnp.where(team == 0, offset(orders[0], place), offset(orders[1], place))
        first = pl.multiple_of((chip ^ shift) * block, block)
        target = (pl.ds(first, block), pl.ds(side * width, width))
        logits[target] = logits[target] + product[number * block : (number + 1) * block]


def load_kernel(source, target, arrival):
    copy = pltpu.make_async_copy(source, target, arrival)
    copy.start()
    copy.wait()


def join_kernel(kept, arrived, out):
    half = kept.shape[0]
    out[:half] = kept[...]
    out[half:] = arrived[...]


def kept_kernel(flows, block, n_chips, targets, kept_a, kept_b, own, other, logits, wanted):
    rows, tokens = wanted.shape[0], targets.shape[1]
    tok_rows = block // targets.shape[0]
    row = lax.broadcasted_iota(jnp.int32, (rows, tokens), 0)
    team = place_of(n_chips)[2]
    token = (2 * (row // block) + (team ^ parity(row // block, n_chips))) * tok_rows + row % tok_rows
    ids = jnp.where(row // tok_rows % 2 == 0, targets[0:1, :], targets[1:2, :])
    here = token == lax.broadcasted_iota(jnp.int32, (rows, tokens), 1)
    wanted[...] = jnp.broadcast_to(jnp.sum(jnp.where(here, ids, 0), axis=1, keepdims=True), wanted.shape)
    logits[...] = jnp.zeros_like(logits)
    for number, (kept, first) in enumerate(((kept_a, 0), (kept_b, kept_a.shape[1]))):
        for side, columns in enumerate((own, other)):
            add_products(flows[number], block, 0, n_chips, kept, columns, side, first, logits)


def first_kernel(flows, block, n_chips, arrived, own, other, partial, logits):
    logits[...] = partial[...]
    for side, columns in enumerate((own, other)):
        add_products(flows[0], block, 1, n_chips, arrived, columns, side, 0, logits)


def stats_kernel(flows, block, n_chips, wanted, arrived, own, other, partial, out, logits):
    device, _, _ = place_of(n_chips)
    width = own.shape[1]
    logits[...] = partial[...]
    for side, columns in enumerate((own, other)):
        add_products(flows[1], block, 1, n_chips, arrived, columns, side, own.shape[0] - arrived.shape[1], logits)
    values = logits[...]
    highest = jnp.max(values, axis=1, keepdims=True)
    exp_total = jnp.sum(jnp.exp(values - highest), axis=1, keepdims=True)
    lane = lax.broadcasted_iota(jnp.int32, values.shape, 1)
    column_ids = jnp.where(lane < width, device * width + lane, (device ^ 1) * width + lane - width)
    picked = jnp.sum(jnp.where(column_ids == wanted[:, :1], values, 0.0), axis=1, keepdims=True)
    member = lax.broadcasted_iota(jnp.int32, (values.shape[0], 128), 1)
    table = jnp.where(member == 0, highest + jnp.log(exp_total), picked)
    out[...] = jnp.transpose(table)[:2]


def pack_kernel(own, other, out):
    for chip_number in range(out.shape[0]):
        out[chip_number, :2] = own[...]
        out[chip_number, 2:] = other[...]


def loss_kernel(n_chips, block, tok_rows, received, own_loss, total):
    chip = place_of(n_chips)[1]
    rows = received.shape[2]
    lane = lax.broadcasted_iota(jnp.int32, (1, rows), 1)
    weight = jnp.where(lane // tok_rows % 2 == 0, 1.0 / rows, MTP_WEIGHT / rows)
    weighted = []
    for first in (2, 0):
        log_sums = received[:, first, :]
        highest = jnp.max(log_sums, axis=0, keepdims=True)
        exp_total = jnp.sum(jnp.exp(log_sums - highest), axis=0, keepdims=True)
        loss = highest + jnp.log(exp_total) - jnp.sum(received[:, first + 1, :], axis=0, keepdims=True)
        weighted.append(loss * weight)
    total[...] = jnp.sum(weighted[0] + weighted[1], axis=1, keepdims=True)
    repeated = jnp.broadcast_to(loss, (8, rows))
    for head in range(2):
        turned = pltpu.roll(repeated, rows - chip * block - head * tok_rows, 1)
        own_loss[pl.ds(head, 1), :] = turned[:1, :tok_rows]


def load(columns):
    return pl.pallas_call(
        load_kernel,
        out_shape=jax.ShapeDtypeStruct(columns.shape, columns.dtype),
        in_specs=[pl.BlockSpec(memory_space=pltpu.HBM)],
        out_specs=pl.BlockSpec(memory_space=pltpu.VMEM),
        scratch_shapes=[pltpu.SemaphoreType.DMA],
        cost_estimate=pl.CostEstimate(flops=0, bytes_accessed=4 * columns.size, transcendentals=0),
        compiler_params=pltpu.CompilerParams(vmem_limit_bytes=2**20 + 2 * columns.size),
    )(columns)


def join(kept, arrived):
    rows, depth = kept.shape
    return pl.pallas_call(
        join_kernel,
        out_shape=jax.ShapeDtypeStruct((2 * rows, depth), kept.dtype),
        cost_estimate=pl.CostEstimate(flops=0, bytes_accessed=8 * kept.size, transcendentals=0),
        compiler_params=pltpu.CompilerParams(vmem_limit_bytes=2**20 + 8 * kept.size),
        name="join",
    )(kept, arrived)


def local(n_vocab, n_chip, hidden, unembed, targets):
    heads, tok_rows, depth = hidden.shape
    block = heads * tok_rows
    width = unembed.shape[1]
    n_chips = n_vocab * n_chip
    flows = gather_orders(n_vocab, n_chip)
    rows = n_chips * block

    other_columns = to_other_core(unembed, n_chips)
    cut = depth // 128 * 2 // 3 * 128
    own_rows = hidden.reshape(block, depth)
    kept = [own_rows[:, :cut], own_rows[:, cut:]]
    arrived = [None, None]
    stages = len(flows[0][0])
    for number in range(stages):
        for flow in range(2):
            masks = (flows[flow][0][number], flows[flow][1][number])
            arrived[flow] = exchange(kept[flow], masks, n_chips)
        if number < stages - 1:
            for flow in range(2):
                kept[flow] = join(kept[flow], arrived[flow])
    own_near, other_near = unembed, load(other_columns)
    cost = pl.CostEstimate(
        flops=2 * rows * width * depth, bytes_accessed=(rows + 4 * width) * depth, transcendentals=0
    )
    held = 2 * (rows + 2 * width) * depth + 4 * rows * (8 * width + 3 * rows + 8 * n_chips)
    params = pltpu.CompilerParams(vmem_limit_bytes=held + 2**21)
    logits = jax.ShapeDtypeStruct((rows, 2 * width), jnp.float32)
    partial, wanted = pl.pallas_call(
        functools.partial(kept_kernel, flows, block, n_chips),
        out_shape=(logits, jax.ShapeDtypeStruct((rows, 128), jnp.int32)),
        cost_estimate=cost,
        compiler_params=params,
        name="kept",
    )(targets, kept[0], kept[1], own_near, other_near)
    partial = pl.pallas_call(
        functools.partial(first_kernel, flows, block, n_chips),
        out_shape=logits,
        cost_estimate=cost,
        compiler_params=params,
        name="first",
    )(arrived[0], own_near, other_near, partial)
    stats = pl.pallas_call(
        functools.partial(stats_kernel, flows, block, n_chips),
        out_shape=jax.ShapeDtypeStruct((2, rows), jnp.float32),
        scratch_shapes=[pltpu.VMEM((rows, 2 * width), jnp.float32)],
        cost_estimate=cost,
        compiler_params=params,
        name="stats",
    )(wanted, arrived[1], own_near, other_near, partial)
    small = pltpu.CompilerParams(vmem_limit_bytes=2**20 + 4 * 4 * n_chips * 8 * rows)
    sent = pl.pallas_call(
        pack_kernel,
        out_shape=jax.ShapeDtypeStruct((n_chips, 4, rows), jnp.float32),
        compiler_params=small,
        name="pack",
    )(stats, to_other_core(stats, n_chips))
    received = lax.all_to_all(
        sent, AXIS, split_axis=0, concat_axis=0, tiled=True, axis_index_groups=team_devices(n_chips)
    )
    token_loss, total = pl.pallas_call(
        functools.partial(loss_kernel, n_chips, block, tok_rows),
        out_shape=(jax.ShapeDtypeStruct((heads, tok_rows), jnp.float32), jax.ShapeDtypeStruct((1, 1), jnp.float32)),
        compiler_params=small,
        name="loss",
    )(received)
    return token_loss, total.reshape(())


def solution(mesh):
    n_vocab, n_data = mesh.shape["vocab"], mesh.shape["dp"]
    line = Mesh(mesh.devices.reshape(-1), (AXIS,))
    return jax.shard_map(
        functools.partial(local, n_vocab, n_data // 2),
        mesh=line,
        in_specs=(P(None, AXIS, None), P(None, AXIS), P()),
        out_specs=(P(None, AXIS), P()),
        check_vma=False,
    )
```

```python
import functools
import jax
import jax.numpy as jnp
from jax import lax
from jax.experimental import pallas as pl
from jax.experimental.pallas import tpu as pltpu
from jax.sharding import Mesh, PartitionSpec as P

MTP_WEIGHT = 0.3
AXIS = "device"


def bits(count):
    return [1 << place for place in range(count.bit_length() - 1)]


def gather_orders(n_vocab, n_chip):
    near = bits(n_chip) + [n_chip * mask for mask in bits(n_vocab)[:1]]
    far = [n_chip * mask for mask in bits(n_vocab)[1:]]
    return (
        (far[::-1] + near[::-1], far + near),
        (near + far, near[::-1] + far[::-1]),
    )


def parity(chip, n_chips):
    odd = chip
    for place in range(1, n_chips.bit_length() - 1):
        odd = odd ^ (chip >> place)
    return odd & 1


def team_devices(n_chips):
    return [[2 * chip + (team ^ parity(chip, n_chips)) for chip in range(n_chips)] for team in range(2)]


def place_of(n_chips):
    device = lax.axis_index(AXIS)
    chip, core = device // 2, device % 2
    return device, chip, core ^ parity(chip, n_chips)


def exchange(value, masks, n_chips):
    teams = team_devices(n_chips)
    pairs = [(teams[team][chip], teams[team][chip ^ masks[team]]) for team in range(2) for chip in range(n_chips)]
    return lax.ppermute(value, AXIS, sorted(pairs))


def to_other_core(value, n_chips):
    pairs = [(source, source ^ 1) for source in range(2 * n_chips)]
    return lax.ppermute(value, AXIS, pairs)


def offset(masks, place):
    total = 0
    for number, mask in enumerate(masks):
        if place >> number & 1:
            total ^= mask
    return total


def add_products(orders, block, part, n_chips, rows, columns, side, first_depth, logits):
    _, chip, team = place_of(n_chips)
    blocks, width = rows.shape[0] // block, columns.shape[1]
    product = jnp.dot(
        rows[...], columns[pl.ds(first_depth, rows.shape[1]), :], preferred_element_type=jnp.float32
    )
    for number in range(blocks):
        place = part * blocks + number
        shift = jnp.where(team == 0, offset(orders[0], place), offset(orders[1], place))
        first = pl.multiple_of((chip ^ shift) * block, block)
        target = (pl.ds(first, block), pl.ds(side * width, width))
        logits[target] = logits[target] + product[number * block : (number + 1) * block]


def load_kernel(source, target, arrival):
    copy = pltpu.make_async_copy(source, target, arrival)
    copy.start()
    copy.wait()


def split_kernel(hidden, out_a, out_b):
    rows = jnp.concatenate([hidden[head] for head in range(hidden.shape[0])], axis=0)
    cut = out_a.shape[1]
    out_a[...] = rows[:, :cut]
    out_b[...] = rows[:, cut:]


def join_kernel(kept, arrived, out):
    half = kept.shape[0]
    out[:half] = kept[...]
    out[half:] = arrived[...]


def kept_kernel(flows, block, n_chips, targets, kept_a, kept_b, own, other, logits, wanted):
    rows, tokens = wanted.shape[0], targets.shape[1]
    tok_rows = block // targets.shape[0]
    row = lax.broadcasted_iota(jnp.int32, (rows, tokens), 0)
    team = place_of(n_chips)[2]
    token = (2 * (row // block) + (team ^ parity(row // block, n_chips))) * tok_rows + row % tok_rows
    ids = jnp.where(row // tok_rows % 2 == 0, targets[0:1, :], targets[1:2, :])
    here = token == lax.broadcasted_iota(jnp.int32, (rows, tokens), 1)
    wanted[...] = jnp.broadcast_to(jnp.sum(jnp.where(here, ids, 0), axis=1, keepdims=True), wanted.shape)
    logits[...] = jnp.zeros_like(logits)
    for number, (kept, first) in enumerate(((kept_a, 0), (kept_b, kept_a.shape[1]))):
        for side, columns in enumerate((own, other)):
            add_products(flows[number], block, 0, n_chips, kept, columns, side, first, logits)


def first_kernel(flows, block, n_chips, arrived, own, other, partial, logits):
    logits[...] = partial[...]
    for side, columns in enumerate((own, other)):
        add_products(flows[0], block, 1, n_chips, arrived, columns, side, 0, logits)


def stats_kernel(flows, block, n_chips, wanted, arrived, own, other, partial, out, logits):
    device, _, _ = place_of(n_chips)
    width = own.shape[1]
    logits[...] = partial[...]
    for side, columns in enumerate((own, other)):
        add_products(flows[1], block, 1, n_chips, arrived, columns, side, own.shape[0] - arrived.shape[1], logits)
    values = logits[...]
    highest = jnp.max(values, axis=1, keepdims=True)
    exp_total = jnp.sum(jnp.exp(values - highest), axis=1, keepdims=True)
    lane = lax.broadcasted_iota(jnp.int32, values.shape, 1)
    column_ids = jnp.where(lane < width, device * width + lane, (device ^ 1) * width + lane - width)
    picked = jnp.sum(jnp.where(column_ids == wanted[:, :1], values, 0.0), axis=1, keepdims=True)
    member = lax.broadcasted_iota(jnp.int32, (values.shape[0], 128), 1)
    table = jnp.where(member == 0, highest + jnp.log(exp_total), picked)
    out[...] = jnp.transpose(table)[:2]


def pack_kernel(own, other, out):
    for chip_number in range(out.shape[0]):
        out[chip_number, :2] = own[...]
        out[chip_number, 2:] = other[...]


def loss_kernel(n_chips, block, tok_rows, received, own_loss, total):
    chip = place_of(n_chips)[1]
    rows = received.shape[2]
    lane = lax.broadcasted_iota(jnp.int32, (1, rows), 1)
    weight = jnp.where(lane // tok_rows % 2 == 0, 1.0 / rows, MTP_WEIGHT / rows)
    weighted = []
    for first in (2, 0):
        log_sums = received[:, first, :]
        highest = jnp.max(log_sums, axis=0, keepdims=True)
        exp_total = jnp.sum(jnp.exp(log_sums - highest), axis=0, keepdims=True)
        loss = highest + jnp.log(exp_total) - jnp.sum(received[:, first + 1, :], axis=0, keepdims=True)
        weighted.append(loss * weight)
    total[...] = jnp.sum(weighted[0] + weighted[1], axis=1, keepdims=True)
    repeated = jnp.broadcast_to(loss, (8, rows))
    for head in range(2):
        turned = pltpu.roll(repeated, rows - chip * block - head * tok_rows, 1)
        own_loss[pl.ds(head, 1), :] = turned[:1, :tok_rows]


def load(columns):
    return pl.pallas_call(
        load_kernel,
        out_shape=jax.ShapeDtypeStruct(columns.shape, columns.dtype),
        in_specs=[pl.BlockSpec(memory_space=pltpu.HBM)],
        out_specs=pl.BlockSpec(memory_space=pltpu.VMEM),
        scratch_shapes=[pltpu.SemaphoreType.DMA],
        cost_estimate=pl.CostEstimate(flops=0, bytes_accessed=4 * columns.size, transcendentals=0),
        compiler_params=pltpu.CompilerParams(vmem_limit_bytes=2**20 + 2 * columns.size),
    )(columns)


def join(kept, arrived):
    rows, depth = kept.shape
    return pl.pallas_call(
        join_kernel,
        out_shape=jax.ShapeDtypeStruct((2 * rows, depth), kept.dtype),
        cost_estimate=pl.CostEstimate(flops=0, bytes_accessed=8 * kept.size, transcendentals=0),
        compiler_params=pltpu.CompilerParams(vmem_limit_bytes=2**20 + 8 * kept.size),
        name="join",
    )(kept, arrived)


def local(n_vocab, n_chip, hidden, unembed, targets):
    heads, tok_rows, depth = hidden.shape
    block = heads * tok_rows
    width = unembed.shape[1]
    n_chips = n_vocab * n_chip
    flows = gather_orders(n_vocab, n_chip)
    rows = n_chips * block

    other_columns = to_other_core(unembed, n_chips)
    cut = depth // 128 * 2 // 3 * 128
    kept = list(
        pl.pallas_call(
            split_kernel,
            out_shape=tuple(jax.ShapeDtypeStruct((block, count), hidden.dtype) for count in (cut, depth - cut)),
            compiler_params=pltpu.CompilerParams(vmem_limit_bytes=2**20 + 8 * hidden.size),
            name="split",
        )(hidden)
    )
    arrived = [None, None]
    stages = len(flows[0][0])
    for number in range(stages):
        for flow in range(2):
            masks = (flows[flow][0][number], flows[flow][1][number])
            arrived[flow] = exchange(kept[flow], masks, n_chips)
        if number < stages - 1:
            for flow in range(2):
                kept[flow] = join(kept[flow], arrived[flow])
    own_near, other_near = unembed, load(other_columns)
    cost = pl.CostEstimate(
        flops=2 * rows * width * depth, bytes_accessed=(rows + 4 * width) * depth, transcendentals=0
    )
    held = 2 * (rows + 2 * width) * depth + 4 * rows * (8 * width + 3 * rows + 8 * n_chips)
    params = pltpu.CompilerParams(vmem_limit_bytes=held + 2**21)
    logits = jax.ShapeDtypeStruct((rows, 2 * width), jnp.float32)
    partial, wanted = pl.pallas_call(
        functools.partial(kept_kernel, flows, block, n_chips),
        out_shape=(logits, jax.ShapeDtypeStruct((rows, 128), jnp.int32)),
        cost_estimate=cost,
        compiler_params=params,
        name="kept",
    )(targets, kept[0], kept[1], own_near, other_near)
    partial = pl.pallas_call(
        functools.partial(first_kernel, flows, block, n_chips),
        out_shape=logits,
        cost_estimate=cost,
        compiler_params=params,
        name="first",
    )(arrived[0], own_near, other_near, partial)
    stats = pl.pallas_call(
        functools.partial(stats_kernel, flows, block, n_chips),
        out_shape=jax.ShapeDtypeStruct((2, rows), jnp.float32),
        scratch_shapes=[pltpu.VMEM((rows, 2 * width), jnp.float32)],
        cost_estimate=cost,
        compiler_params=params,
        name="stats",
    )(wanted, arrived[1], own_near, other_near, partial)
    small = pltpu.CompilerParams(vmem_limit_bytes=2**20 + 4 * 4 * n_chips * 8 * rows)
    sent = pl.pallas_call(
        pack_kernel,
        out_shape=jax.ShapeDtypeStruct((n_chips, 4, rows), jnp.float32),
        compiler_params=small,
        name="pack",
    )(stats, to_other_core(stats, n_chips))
    received = lax.all_to_all(
        sent, AXIS, split_axis=0, concat_axis=0, tiled=True, axis_index_groups=team_devices(n_chips)
    )
    token_loss, total = pl.pallas_call(
        functools.partial(loss_kernel, n_chips, block, tok_rows),
        out_shape=(jax.ShapeDtypeStruct((heads, tok_rows), jnp.float32), jax.ShapeDtypeStruct((1, 1), jnp.float32)),
        compiler_params=small,
        name="loss",
    )(received)
    return token_loss, total.reshape(())


def solution(mesh):
    n_vocab, n_data = mesh.shape["vocab"], mesh.shape["dp"]
    line = Mesh(mesh.devices.reshape(-1), (AXIS,))
    return jax.shard_map(
        functools.partial(local, n_vocab, n_data // 2),
        mesh=line,
        in_specs=(P(None, AXIS, None), P(None, AXIS), P()),
        out_specs=(P(None, AXIS), P()),
        check_vma=False,
    )
```

```python
import functools
import jax
import jax.numpy as jnp
from jax import lax
from jax.experimental import pallas as pl
from jax.experimental.pallas import tpu as pltpu
from jax.sharding import Mesh, PartitionSpec as P

MTP_WEIGHT = 0.3
AXIS = "device"


def bits(count):
    return [1 << place for place in range(count.bit_length() - 1)]


def gather_orders(n_vocab, n_chip):
    near = bits(n_chip) + [n_chip * mask for mask in bits(n_vocab)[:1]]
    far = [n_chip * mask for mask in bits(n_vocab)[1:]]
    return (
        (far[::-1] + near[::-1], far + near),
        (near[::-1] + far, near + far[::-1]),
    )


def parity(chip, chips):
    line = chip // chips[1]
    odd = line
    for place in range(1, chips[0].bit_length() - 1):
        odd = odd ^ (line >> place)
    return odd & 1


def team_devices(chips):
    return [[2 * chip + (team ^ parity(chip, chips)) for chip in range(chips[0] * chips[1])] for team in range(2)]


def place_of(chips):
    device = lax.axis_index(AXIS)
    chip, core = device // 2, device % 2
    return device, chip, core ^ parity(chip, chips)


def exchange(value, masks, chips):
    teams = team_devices(chips)
    pairs = [(teams[team][chip], teams[team][chip ^ masks[team]]) for team in range(2) for chip in range(chips[0] * chips[1])]
    return lax.ppermute(value, AXIS, sorted(pairs))


def to_other_core(value, n_chips):
    pairs = [(source, source ^ 1) for source in range(2 * n_chips)]
    return lax.ppermute(value, AXIS, pairs)


def offset(masks, place):
    total = 0
    for number, mask in enumerate(masks):
        if place >> number & 1:
            total ^= mask
    return total


def add_products(orders, block, part, chips, rows, columns, side, first_depth, logits):
    _, chip, team = place_of(chips)
    blocks, width = rows.shape[0] // block, columns.shape[1]
    product = jnp.dot(
        rows[...], columns[pl.ds(first_depth, rows.shape[1]), :], preferred_element_type=jnp.float32
    )
    for number in range(blocks):
        place = part * blocks + number
        shift = jnp.where(team == 0, offset(orders[0], place), offset(orders[1], place))
        first = pl.multiple_of((chip ^ shift) * block, block)
        target = (pl.ds(first, block), pl.ds(side * width, width))
        logits[target] = logits[target] + product[number * block : (number + 1) * block]


def load_kernel(source, target, arrival):
    copy = pltpu.make_async_copy(source, target, arrival)
    copy.start()
    copy.wait()


def split_kernel(hidden, out_a, out_b):
    rows = jnp.concatenate([hidden[head] for head in range(hidden.shape[0])], axis=0)
    cut = out_a.shape[1]
    out_a[...] = rows[:, :cut]
    out_b[...] = rows[:, cut:]


def join_kernel(kept, arrived, out):
    half = kept.shape[0]
    out[:half] = kept[...]
    out[half:] = arrived[...]


def kept_kernel(flows, block, chips, targets, kept_a, kept_b, own, other, logits, wanted):
    rows, tokens = wanted.shape[0], targets.shape[1]
    tok_rows = block // targets.shape[0]
    row = lax.broadcasted_iota(jnp.int32, (rows, tokens), 0)
    team = place_of(chips)[2]
    token = (2 * (row // block) + (team ^ parity(row // block, chips))) * tok_rows + row % tok_rows
    ids = jnp.where(row // tok_rows % 2 == 0, targets[0:1, :], targets[1:2, :])
    here = token == lax.broadcasted_iota(jnp.int32, (rows, tokens), 1)
    wanted[...] = jnp.broadcast_to(jnp.sum(jnp.where(here, ids, 0), axis=1, keepdims=True), wanted.shape)
    logits[...] = jnp.zeros_like(logits)
    for number, (kept, first) in enumerate(((kept_a, 0), (kept_b, kept_a.shape[1]))):
        for side, columns in enumerate((own, other)):
            add_products(flows[number], block, 0, chips, kept, columns, side, first, logits)


def first_kernel(flows, block, chips, arrived, own, other, partial, logits):
    logits[...] = partial[...]
    for side, columns in enumerate((own, other)):
        add_products(flows[0], block, 1, chips, arrived, columns, side, 0, logits)


def stats_kernel(flows, block, chips, wanted, arrived, own, other, partial, out, logits):
    device, _, _ = place_of(chips)
    width = own.shape[1]
    logits[...] = partial[...]
    for side, columns in enumerate((own, other)):
        add_products(flows[1], block, 1, chips, arrived, columns, side, own.shape[0] - arrived.shape[1], logits)
    values = logits[...]
    highest = jnp.max(values, axis=1, keepdims=True)
    exp_total = jnp.sum(jnp.exp(values - highest), axis=1, keepdims=True)
    lane = lax.broadcasted_iota(jnp.int32, values.shape, 1)
    column_ids = jnp.where(lane < width, device * width + lane, (device ^ 1) * width + lane - width)
    picked = jnp.sum(jnp.where(column_ids == wanted[:, :1], values, 0.0), axis=1, keepdims=True)
    member = lax.broadcasted_iota(jnp.int32, (values.shape[0], 128), 1)
    table = jnp.where(member == 0, highest + jnp.log(exp_total), picked)
    out[...] = jnp.transpose(table)[:2]


def pack_kernel(own, other, out):
    for chip_number in range(out.shape[0]):
        out[chip_number, :2] = own[...]
        out[chip_number, 2:] = other[...]


def loss_kernel(chips, block, tok_rows, received, own_loss, total):
    chip = place_of(chips)[1]
    rows = received.shape[2]
    lane = lax.broadcasted_iota(jnp.int32, (1, rows), 1)
    weight = jnp.where(lane // tok_rows % 2 == 0, 1.0 / rows, MTP_WEIGHT / rows)
    weighted = []
    for first in (2, 0):
        log_sums = received[:, first, :]
        highest = jnp.max(log_sums, axis=0, keepdims=True)
        exp_total = jnp.sum(jnp.exp(log_sums - highest), axis=0, keepdims=True)
        loss = highest + jnp.log(exp_total) - jnp.sum(received[:, first + 1, :], axis=0, keepdims=True)
        weighted.append(loss * weight)
    total[...] = jnp.sum(weighted[0] + weighted[1], axis=1, keepdims=True)
    repeated = jnp.broadcast_to(loss, (8, rows))
    for head in range(2):
        turned = pltpu.roll(repeated, rows - chip * block - head * tok_rows, 1)
        own_loss[pl.ds(head, 1), :] = turned[:1, :tok_rows]


def load(columns):
    return pl.pallas_call(
        load_kernel,
        out_shape=jax.ShapeDtypeStruct(columns.shape, columns.dtype),
        in_specs=[pl.BlockSpec(memory_space=pltpu.HBM)],
        out_specs=pl.BlockSpec(memory_space=pltpu.VMEM),
        scratch_shapes=[pltpu.SemaphoreType.DMA],
        cost_estimate=pl.CostEstimate(flops=0, bytes_accessed=4 * columns.size, transcendentals=0),
        compiler_params=pltpu.CompilerParams(vmem_limit_bytes=2**20 + 2 * columns.size),
    )(columns)


def join(kept, arrived):
    rows, depth = kept.shape
    return pl.pallas_call(
        join_kernel,
        out_shape=jax.ShapeDtypeStruct((2 * rows, depth), kept.dtype),
        cost_estimate=pl.CostEstimate(flops=0, bytes_accessed=8 * kept.size, transcendentals=0),
        compiler_params=pltpu.CompilerParams(vmem_limit_bytes=2**20 + 8 * kept.size),
        name="join",
    )(kept, arrived)


def local(n_vocab, n_chip, hidden, unembed, targets):
    heads, tok_rows, depth = hidden.shape
    block = heads * tok_rows
    width = unembed.shape[1]
    chips = (n_vocab, n_chip)
    n_chips = n_vocab * n_chip
    flows = gather_orders(n_vocab, n_chip)
    rows = n_chips * block

    other_columns = to_other_core(unembed, n_chips)
    cut = depth // 128 * 2 // 3 * 128
    kept = list(
        pl.pallas_call(
            split_kernel,
            out_shape=tuple(jax.ShapeDtypeStruct((block, count), hidden.dtype) for count in (cut, depth - cut)),
            compiler_params=pltpu.CompilerParams(vmem_limit_bytes=2**20 + 8 * hidden.size),
            name="split",
        )(hidden)
    )
    arrived = [None, None]
    stages = len(flows[0][0])
    for number in range(stages):
        for flow in range(2):
            masks = (flows[flow][0][number], flows[flow][1][number])
            arrived[flow] = exchange(kept[flow], masks, chips)
        if number < stages - 1:
            for flow in range(2):
                kept[flow] = join(kept[flow], arrived[flow])
    own_near, other_near = unembed, load(other_columns)
    cost = pl.CostEstimate(
        flops=2 * rows * width * depth, bytes_accessed=(rows + 4 * width) * depth, transcendentals=0
    )
    held = 2 * (rows + 2 * width) * depth + 4 * rows * (8 * width + 3 * rows + 8 * n_chips)
    params = pltpu.CompilerParams(vmem_limit_bytes=held + 2**21)
    logits = jax.ShapeDtypeStruct((rows, 2 * width), jnp.float32)
    partial, wanted = pl.pallas_call(
        functools.partial(kept_kernel, flows, block, chips),
        out_shape=(logits, jax.ShapeDtypeStruct((rows, 128), jnp.int32)),
        cost_estimate=cost,
        compiler_params=params,
        name="kept",
    )(targets, kept[0], kept[1], own_near, other_near)
    partial = pl.pallas_call(
        functools.partial(first_kernel, flows, block, chips),
        out_shape=logits,
        cost_estimate=cost,
        compiler_params=params,
        name="first",
    )(arrived[0], own_near, other_near, partial)
    stats = pl.pallas_call(
        functools.partial(stats_kernel, flows, block, chips),
        out_shape=jax.ShapeDtypeStruct((2, rows), jnp.float32),
        scratch_shapes=[pltpu.VMEM((rows, 2 * width), jnp.float32)],
        cost_estimate=cost,
        compiler_params=params,
        name="stats",
    )(wanted, arrived[1], own_near, other_near, partial)
    small = pltpu.CompilerParams(vmem_limit_bytes=2**20 + 4 * 4 * n_chips * 8 * rows)
    sent = pl.pallas_call(
        pack_kernel,
        out_shape=jax.ShapeDtypeStruct((n_chips, 4, rows), jnp.float32),
        compiler_params=small,
        name="pack",
    )(stats, to_other_core(stats, n_chips))
    order = list(range(n_chips))[::-1]
    received = lax.all_to_all(
        sent, AXIS, split_axis=0, concat_axis=0, tiled=True, axis_index_groups=[[team[c] for c in order] for team in team_devices(chips)]
    )
    token_loss, total = pl.pallas_call(
        functools.partial(loss_kernel, chips, block, tok_rows),
        out_shape=(jax.ShapeDtypeStruct((heads, tok_rows), jnp.float32), jax.ShapeDtypeStruct((1, 1), jnp.float32)),
        compiler_params=small,
        name="loss",
    )(received)
    return token_loss, total.reshape(())


def solution(mesh):
    n_vocab, n_data = mesh.shape["vocab"], mesh.shape["dp"]
    line = Mesh(mesh.devices.reshape(-1), (AXIS,))
    return jax.shard_map(
        functools.partial(local, n_vocab, n_data // 2),
        mesh=line,
        in_specs=(P(None, AXIS, None), P(None, AXIS), P()),
        out_specs=(P(None, AXIS), P()),
        check_vma=False,
    )
```

```python
import functools
import jax
import jax.numpy as jnp
from jax import lax
from jax.experimental import pallas as pl
from jax.experimental.pallas import tpu as pltpu
from jax.sharding import Mesh, PartitionSpec as P

MTP_WEIGHT = 0.3
AXIS = "device"


def bits(count):
    return [1 << place for place in range(count.bit_length() - 1)]


def gather_orders(n_vocab, n_chip):
    near = bits(n_chip) + [n_chip * mask for mask in bits(n_vocab)[:1]]
    far = [n_chip * mask for mask in bits(n_vocab)[1:]]
    return (
        (far[::-1] + near[::-1], far + near),
        (near[::-1] + far, near + far[::-1]),
    )


def parity(chip, chips):
    line = chip // chips[1]
    odd = line
    for place in range(1, chips[0].bit_length() - 1):
        odd = odd ^ (line >> place)
    return odd & 1


def team_devices(chips):
    return [[2 * chip + (team ^ parity(chip, chips)) for chip in range(chips[0] * chips[1])] for team in range(2)]


def place_of(chips):
    device = lax.axis_index(AXIS)
    chip, core = device // 2, device % 2
    return device, chip, core ^ parity(chip, chips)


def exchange(value, masks, chips):
    teams = team_devices(chips)
    pairs = [(teams[team][chip], teams[team][chip ^ masks[team]]) for team in range(2) for chip in range(chips[0] * chips[1])]
    return lax.ppermute(value, AXIS, sorted(pairs))


def to_other_core(value, n_chips):
    pairs = [(source, source ^ 1) for source in range(2 * n_chips)]
    return lax.ppermute(value, AXIS, pairs)


def offset(masks, place):
    total = 0
    for number, mask in enumerate(masks):
        if place >> number & 1:
            total ^= mask
    return total


def add_products(orders, block, part, chips, rows, columns, side, first_depth, logits):
    _, chip, team = place_of(chips)
    blocks, width = rows.shape[0] // block, columns.shape[1]
    product = jnp.dot(
        rows[...], columns[pl.ds(first_depth, rows.shape[1]), :], preferred_element_type=jnp.float32
    )
    for number in range(blocks):
        place = part * blocks + number
        shift = jnp.where(team == 0, offset(orders[0], place), offset(orders[1], place))
        first = pl.multiple_of((chip ^ shift) * block, block)
        target = (pl.ds(first, block), pl.ds(side * width, width))
        logits[target] = logits[target] + product[number * block : (number + 1) * block]


def split_kernel(hidden, out_a, out_b):
    rows = jnp.concatenate([hidden[head] for head in range(hidden.shape[0])], axis=0)
    cut = out_a.shape[1]
    out_a[...] = rows[:, :cut]
    out_b[...] = rows[:, cut:]


def join_kernel(kept, arrived, out):
    half = kept.shape[0]
    out[:half] = kept[...]
    out[half:] = arrived[...]


def kept_kernel(flows, block, chips, targets, kept_a, kept_b, own, other, logits, wanted):
    rows, tokens = wanted.shape[0], targets.shape[1]
    tok_rows = block // targets.shape[0]
    row = lax.broadcasted_iota(jnp.int32, (rows, tokens), 0)
    team = place_of(chips)[2]
    token = (2 * (row // block) + (team ^ parity(row // block, chips))) * tok_rows + row % tok_rows
    ids = jnp.where(row // tok_rows % 2 == 0, targets[0:1, :], targets[1:2, :])
    here = token == lax.broadcasted_iota(jnp.int32, (rows, tokens), 1)
    wanted[...] = jnp.broadcast_to(jnp.sum(jnp.where(here, ids, 0), axis=1, keepdims=True), wanted.shape)
    logits[...] = jnp.zeros_like(logits)
    for number, (kept, first) in enumerate(((kept_a, 0), (kept_b, kept_a.shape[1]))):
        for side, columns in enumerate((own, other)):
            add_products(flows[number], block, 0, chips, kept, columns, side, first, logits)


def first_kernel(flows, block, chips, arrived, own, other, partial, logits):
    for side, columns in enumerate((own, other)):
        add_products(flows[0], block, 1, chips, arrived, columns, side, 0, logits)


def stats_kernel(flows, block, chips, wanted, arrived, own, other, partial, out, logits):
    device, _, _ = place_of(chips)
    width = own.shape[1]
    for side, columns in enumerate((own, other)):
        add_products(flows[1], block, 1, chips, arrived, columns, side, own.shape[0] - arrived.shape[1], logits)
    values = logits[...]
    highest = jnp.max(values, axis=1, keepdims=True)
    exp_total = jnp.sum(jnp.exp(values - highest), axis=1, keepdims=True)
    lane = lax.broadcasted_iota(jnp.int32, values.shape, 1)
    column_ids = jnp.where(lane < width, device * width + lane, (device ^ 1) * width + lane - width)
    picked = jnp.sum(jnp.where(column_ids == wanted[:, :1], values, 0.0), axis=1, keepdims=True)
    member = lax.broadcasted_iota(jnp.int32, (values.shape[0], 128), 1)
    table = jnp.where(member == 0, highest + jnp.log(exp_total), picked)
    out[...] = jnp.transpose(table)[:2]


def pack_kernel(own, other, out):
    for chip_number in range(out.shape[0]):
        out[chip_number, :2] = own[...]
        out[chip_number, 2:] = other[...]


def loss_kernel(chips, block, tok_rows, received, own_loss, total):
    chip = place_of(chips)[1]
    rows = received.shape[2]
    lane = lax.broadcasted_iota(jnp.int32, (1, rows), 1)
    weight = jnp.where(lane // tok_rows % 2 == 0, 1.0 / rows, MTP_WEIGHT / rows)
    weighted = []
    for first in (2, 0):
        log_sums = received[:, first, :]
        highest = jnp.max(log_sums, axis=0, keepdims=True)
        exp_total = jnp.sum(jnp.exp(log_sums - highest), axis=0, keepdims=True)
        loss = highest + jnp.log(exp_total) - jnp.sum(received[:, first + 1, :], axis=0, keepdims=True)
        weighted.append(loss * weight)
    total[...] = jnp.sum(weighted[0] + weighted[1], axis=1, keepdims=True)
    repeated = jnp.broadcast_to(loss, (8, rows))
    for head in range(2):
        turned = pltpu.roll(repeated, rows - chip * block - head * tok_rows, 1)
        own_loss[pl.ds(head, 1), :] = turned[:1, :tok_rows]


def join(kept, arrived):
    rows, depth = kept.shape
    return pl.pallas_call(
        join_kernel,
        out_shape=jax.ShapeDtypeStruct((2 * rows, depth), kept.dtype),
        cost_estimate=pl.CostEstimate(flops=0, bytes_accessed=8 * kept.size, transcendentals=0),
        compiler_params=pltpu.CompilerParams(vmem_limit_bytes=2**20 + 8 * kept.size),
        name="join",
    )(kept, arrived)


def local(n_vocab, n_chip, hidden, unembed, targets):
    heads, tok_rows, depth = hidden.shape
    block = heads * tok_rows
    width = unembed.shape[1]
    chips = (n_vocab, n_chip)
    n_chips = n_vocab * n_chip
    flows = gather_orders(n_vocab, n_chip)
    rows = n_chips * block

    other_columns = to_other_core(unembed, n_chips)
    cut = depth // 128 * 2 // 3 * 128
    kept = list(
        pl.pallas_call(
            split_kernel,
            out_shape=tuple(jax.ShapeDtypeStruct((block, count), hidden.dtype) for count in (cut, depth - cut)),
            compiler_params=pltpu.CompilerParams(vmem_limit_bytes=2**20 + 8 * hidden.size),
            name="split",
        )(hidden)
    )
    arrived = [None, None]
    stages = len(flows[0][0])
    for number in range(stages):
        for flow in range(2):
            masks = (flows[flow][0][number], flows[flow][1][number])
            arrived[flow] = exchange(kept[flow], masks, chips)
        if number < stages - 1:
            for flow in range(2):
                kept[flow] = join(kept[flow], arrived[flow])
    cost = pl.CostEstimate(
        flops=2 * rows * width * depth, bytes_accessed=(rows + 4 * width) * depth, transcendentals=0
    )
    held = 2 * (rows + 2 * width) * depth + 4 * rows * (8 * width + 3 * rows + 8 * n_chips)
    params = pltpu.CompilerParams(vmem_limit_bytes=held + 2**21)
    logits = jax.ShapeDtypeStruct((rows, 2 * width), jnp.float32)
    partial, wanted = pl.pallas_call(
        functools.partial(kept_kernel, flows, block, chips),
        out_shape=(logits, jax.ShapeDtypeStruct((rows, 128), jnp.int32)),
        cost_estimate=cost,
        compiler_params=params,
        name="kept",
    )(targets, kept[0], kept[1], unembed, other_columns)
    partial = pl.pallas_call(
        functools.partial(first_kernel, flows, block, chips),
        out_shape=logits,
        cost_estimate=cost,
        compiler_params=params,
        input_output_aliases={3: 0},
        name="first",
    )(arrived[0], unembed, other_columns, partial)
    stats, _ = pl.pallas_call(
        functools.partial(stats_kernel, flows, block, chips),
        out_shape=(jax.ShapeDtypeStruct((2, rows), jnp.float32), logits),
        cost_estimate=cost,
        compiler_params=params,
        input_output_aliases={4: 1},
        name="stats",
    )(wanted, arrived[1], unembed, other_columns, partial)
    small = pltpu.CompilerParams(vmem_limit_bytes=2**20 + 4 * 4 * n_chips * 8 * rows)
    sent = pl.pallas_call(
        pack_kernel,
        out_shape=jax.ShapeDtypeStruct((n_chips, 4, rows), jnp.float32),
        compiler_params=small,
        name="pack",
    )(stats, to_other_core(stats, n_chips))
    order = list(range(n_chips))[::-1]
    received = lax.all_to_all(
        sent, AXIS, split_axis=0, concat_axis=0, tiled=True, axis_index_groups=[[team[c] for c in order] for team in team_devices(chips)]
    )
    token_loss, total = pl.pallas_call(
        functools.partial(loss_kernel, chips, block, tok_rows),
        out_shape=(jax.ShapeDtypeStruct((heads, tok_rows), jnp.float32), jax.ShapeDtypeStruct((1, 1), jnp.float32)),
        compiler_params=small,
        name="loss",
    )(received)
    return token_loss, total.reshape(())


def solution(mesh):
    n_vocab, n_data = mesh.shape["vocab"], mesh.shape["dp"]
    line = Mesh(mesh.devices.reshape(-1), (AXIS,))
    return jax.shard_map(
        functools.partial(local, n_vocab, n_data // 2),
        mesh=line,
        in_specs=(P(None, AXIS, None), P(None, AXIS), P()),
        out_specs=(P(None, AXIS), P()),
        check_vma=False,
    )
```
